16 devices in a mesh: dp: 2 (over y, z), tp: 8 (over x, core).
Axes of the slice: x: 4, y: 2, z: 1, core: 2. Of those that a mesh axis runs over, the one named last changes fastest.
The devices are a block of a 4x4x8 slice.
Arguments:
- x: bfloat16 [8, 512, 6144], P('dp'), parts along dimension 0
- gain_a: bfloat16 [6144], replicated
- wq: bfloat16 [6144, 6144], P(None, 'tp')
- wk: bfloat16 [6144, 1024], P(None, 'tp')
- wv: bfloat16 [6144, 1024], P(None, 'tp')
- wo: bfloat16 [6144, 6144], P('tp')
- gain_m: bfloat16 [6144], replicated
- w_gate: bfloat16 [6144, 16384], P(None, 'tp')
- w_up: bfloat16 [6144, 16384], P(None, 'tp')
- w_down: bfloat16 [16384, 6144], P('tp')
Outputs:
- output: bfloat16 [8, 512, 6144], P('dp'), parts along dimension 0
There are 2 independent parts. The reference program is written for one: setup_inputs(seed, part) draws one part's arguments, and reference() takes and returns one part's arrays. A program takes and returns all parts, laid end to end along the dimension named above; an argument that names none is the same for every part.
All inputs are finite; a program needn't handle non-finite values.
Results may differ from the reference program's by a relative error of at most 0.017.
Values are sent between devices in bfloat16 or wider.
A program may use at most 768 MiB of HBM per device.

```python
import jax
import jax.numpy as jnp
from jax import lax

SEQUENCES = 4
TOKENS = 512
D = 6144
HEADS = 48
KV_HEADS = 8
HEAD = 128
FF = 16384
THETA = 10000


def setup_inputs(seed: int = 0, part: int = 0) -> dict:
    kx, ka, km, kq, kk, kv, ko, kg, ku, kd = jax.random.split(jax.random.key(seed), 10)

    def weights(key, rows, columns):
        return jax.random.normal(key, (rows, columns), jnp.float32) * rows**-0.5

    drawn = {
        "x": jax.random.normal(jax.random.fold_in(kx, part), (SEQUENCES, TOKENS, D), jnp.float32),
        "gain_a": 1 + 0.1 * jax.random.normal(ka, (D,), jnp.float32),
        "wq": 2 * weights(kq, D, HEADS * HEAD),
        "wk": 2 * weights(kk, D, KV_HEADS * HEAD),
        "wv": 4 * weights(kv, D, KV_HEADS * HEAD),
        "wo": weights(ko, HEADS * HEAD, D),
        "gain_m": 1 + 0.1 * jax.random.normal(km, (D,), jnp.float32),
        "w_gate": weights(kg, D, FF),
        "w_up": weights(ku, D, FF),
        "w_down": 3 * weights(kd, FF, D),
    }
    return {k: v.astype(jnp.bfloat16) for k, v in drawn.items()}


def normed(x, gain):
    wide = x.astype(jnp.float32)
    scale = lax.rsqrt(jnp.mean(wide * wide, -1, keepdims=True) + 1e-6)
    return (wide * scale * gain.astype(jnp.float32)).astype(jnp.bfloat16)


def turned(t, place, theta):
    half = t.shape[-1] // 2
    angle = place.astype(jnp.float32)[:, None] * theta ** (-jnp.arange(half, dtype=jnp.float32) / half)
    cos, sin = jnp.cos(angle)[:, None], jnp.sin(angle)[:, None]
    a, b = t[..., :half].astype(jnp.float32), t[..., half:].astype(jnp.float32)
    return jnp.concatenate([a * cos - b * sin, b * cos + a * sin], -1).astype(jnp.bfloat16)


def matmul(a, w):
    return jnp.dot(a, w, preferred_element_type=jnp.float32).astype(jnp.bfloat16)


def einsum(form, a, b):
    return jnp.einsum(form, a.astype(jnp.float32), b.astype(jnp.float32))


def attention(q, k, v):
    scores = einsum("tgsd,ugd->gstu", q, k) * q.shape[-1] ** -0.5
    token = jnp.arange(q.shape[0])
    scores = jnp.where(token[:, None] >= token, scores, -jnp.inf)
    weights = jax.nn.softmax(scores, -1).astype(jnp.bfloat16)
    return einsum("gstu,ugd->tgsd", weights, v).astype(jnp.bfloat16)


def one(x, gain_a, wq, wk, wv, wo, gain_m, w_gate, w_up, w_down):
    rows = x.shape[0]
    a, place = normed(x, gain_a), jnp.arange(rows)
    k = turned(matmul(a, wk).reshape(rows, -1, HEAD), place, THETA)
    q = turned(matmul(a, wq).reshape(rows, -1, HEAD), place, THETA).reshape(rows, k.shape[1], -1, HEAD)
    v = matmul(a, wv).reshape(rows, -1, HEAD)
    seen = attention(q, k, v).reshape(rows, -1)
    h = (x.astype(jnp.float32) + jnp.dot(seen, wo, preferred_element_type=jnp.float32)).astype(jnp.bfloat16)
    b = normed(h, gain_m)
    gate = jnp.dot(b, w_gate, preferred_element_type=jnp.float32)
    up = jnp.dot(b, w_up, preferred_element_type=jnp.float32)
    hidden = (jax.nn.silu(gate) * up).astype(jnp.bfloat16)
    return (h.astype(jnp.float32) + jnp.dot(hidden, w_down, preferred_element_type=jnp.float32)).astype(jnp.bfloat16)


def reference(x, gain_a, wq, wk, wv, wo, gain_m, w_gate, w_up, w_down):
    return lax.map(lambda sequence: one(sequence, gain_a, wq, wk, wv, wo, gain_m, w_gate, w_up, w_down), x)
```

```python
import functools

import jax
import jax.numpy as jnp
from jax import lax
from jax.experimental import pallas as pl
from jax.experimental.pallas import tpu as pltpu
from jax.sharding import PartitionSpec as P

HEAD = 128
THETA = 10000
EPS = 1e-6
WIDE = 256
OUT = 512
BF16, F32 = jnp.bfloat16, jnp.float32
MESH = pl.DeviceIdType.MESH
D2D, FAR_A, NEAR_B, FAR_B, NEAR_A, RUN_A, RUN_B, RIGHT, LEFT, SIDE, FWD_A, FWD_B, SIDE_L, SIDE_R, SIDE_2 = range(15)


def _dot(a, b):
    return jnp.dot(a, b, preferred_element_type=F32)


def _layer(x_ref, gain_a, gain_m, cos_ref, sin_ref, wq, wk, wv, wo, w_gate, w_up, w_down, g_ref,
           xb, wbuf, dbuf, own, oth, sib, hid, gate_s, rsr, sbuf, sf, hrow, stage,
           send, recv, xsem, wsem, vsem, dsem, hsem, lsem):
    n_seq, tokens, d = x_ref.shape
    chips, rows = g_ref.shape[1], g_ref.shape[3]
    half = rows // 2
    split = chips * rows
    qw, ff = wq.shape[1], w_down.shape[0]
    heads = qw // HEAD
    k_at, v_at, seen_at = qw, qw + HEAD, qw + 2 * HEAD
    n_wide, n_out = qw // WIDE + 1, d // OUT
    n_ff = ff // WIDE
    chunk = d // 4

    at = lax.axis_index("tp")
    me, core = at // 2, lax.rem(at, 2)
    rel = lambda k: lax.rem(me + k, chips)
    device = lambda chip: {"tp": chip * 2 + core}
    right, left, other = device(rel(1)), device(rel(chips - 1)), {"tp": me * 2 + 1 - core}

    def x_copy(s):
        return pltpu.make_async_copy(x_ref.at[s], xb, xsem.at[2 * chips])

    def b_copies(m):
        return [pltpu.make_async_copy(g_ref.at[m, k, core if j == 0 else 1 - core], xb.at[pl.ds(j * split + k * rows, rows)],
                                      xsem.at[j * chips + k]) for j in range(2) for k in range(chips)]

    def row_copy(s):
        return pltpu.make_async_copy(x_ref.at[s, pl.ds(pl.multiple_of(at * rows, rows), rows)], hrow.at[s], hsem.at[s])

    def tile(w, n, slot):
        return pltpu.make_async_copy(w.at[:, pl.ds(pl.multiple_of(n * WIDE, WIDE), WIDE)], wbuf.at[slot], wsem.at[slot])

    def kv(slot):
        return (pltpu.make_async_copy(wk, wbuf.at[slot, :, pl.ds(0, HEAD)], vsem.at[0]),
                pltpu.make_async_copy(wv, wbuf.at[slot, :, pl.ds(HEAD, HEAD)], vsem.at[1]))

    def on_qkv(n, act):
        slot = lax.rem(n, 2)

        @pl.when(n < n_wide - 1)
        def _():
            act(tile(wq, n, slot))

        @pl.when(n == n_wide - 1)
        def _():
            for copy in kv(slot):
                act(copy)

    def out_tile(w, n):
        slot = lax.rem(n, 2)
        return pltpu.make_async_copy(w.at[:, pl.ds(pl.multiple_of(n * OUT, OUT), OUT)], dbuf.at[slot, pl.ds(0, w.shape[0])], dsem.at[slot])

    start, wait = lambda copy: copy.start(), lambda copy: copy.wait()

    def message(kind, t, src, dst, to):
        return pltpu.make_async_remote_copy(src_ref=src, dst_ref=dst, send_sem=send.at[kind, t], recv_sem=recv.at[kind, t],
                                            device_id=to, device_id_type=MESH)

    def sent(kind, t):
        par = lax.rem(t, 2)
        part_a, part_b = pl.ds(0, half), pl.ds(half, half)
        if kind == D2D:
            return message(kind, t, oth, sib.at[par], other)
        if kind in (FAR_A, NEAR_B, FAR_B, NEAR_A):
            k = kind - FAR_A
            return message(kind, t, sbuf.at[k], rsr.at[par, k], right if k < 2 else left)
        if kind == RUN_A:
            return message(kind, t, rsr.at[par, 0], rsr.at[par, 4], right)
        if kind == RUN_B:
            return message(kind, t, rsr.at[par, 2], rsr.at[par, 5], left)
        mine = g_ref.at[t, me, core]
        if kind in (RIGHT, LEFT, SIDE):
            return message(kind, t, stage.at[par], mine, {RIGHT: right, LEFT: left, SIDE: other}[kind])
        if kind == FWD_A:
            ref = g_ref.at[t, rel(chips - 1), core, part_a]
            return message(kind, t, ref, ref, right)
        if kind == FWD_B:
            ref = g_ref.at[t, rel(1), core, part_b]
            return message(kind, t, ref, ref, left)
        ref = g_ref.at[t, rel({SIDE_L: chips - 1, SIDE_R: 1, SIDE_2: 2}[kind]), core]
        return message(kind, t, ref, ref, other)

    def arrived(kind, t):
        par = lax.rem(t, 2)
        part_a, part_b = pl.ds(0, half), pl.ds(half, half)
        if kind == D2D:
            ref, who = sib.at[par], other
        elif kind in (FAR_A, NEAR_B, FAR_B, NEAR_A):
            k = kind - FAR_A
            ref, who = rsr.at[par, k], (left if k < 2 else right)
        elif kind == RUN_A:
            ref, who = rsr.at[par, 4], left
        elif kind == RUN_B:
            ref, who = rsr.at[par, 5], right
        elif kind == RIGHT:
            ref, who = g_ref.at[t, rel(chips - 1), core], left
        elif kind == LEFT:
            ref, who = g_ref.at[t, rel(1), core], right
        elif kind == FWD_A:
            ref, who = g_ref.at[t, rel(2), core, part_a], left
        elif kind == FWD_B:
            ref, who = g_ref.at[t, rel(2), core, part_b], right
        else:
            ref, who = g_ref.at[t, rel({SIDE: 0, SIDE_L: chips - 1, SIDE_R: 1, SIDE_2: 2}[kind]), 1 - core], other
        message(kind, t, ref, ref, who).wait_recv()

    def go(kind, t):
        sent(kind, t).start()

    def gone(kind, t):
        sent(kind, t).wait_send()

    def mine_copy(t):
        return pltpu.make_async_copy(stage.at[lax.rem(t, 2)], g_ref.at[t, me, core], lsem.at[t])

    def spread(t):
        par = lax.rem(t, 2)
        gone(D2D, t)
        arrived(D2D, t)

        @pl.when(t >= 1)
        def _():
            for kind in (FAR_A, NEAR_B, FAR_B, NEAR_A):
                gone(kind, t - 1)

        def add(k, part, to, slot):
            base = rel(k) * rows + part * half

            @pl.loop(0, half // 16)
            def _(i):
                here = pl.ds(pl.multiple_of(base + i * 16, 16), 16)
                for c in range(0, d, chunk):
                    total = own[here, c : c + chunk] + sib[par, here, c : c + chunk].astype(F32)
                    to[slot, pl.ds(i * 16, 16), c : c + chunk] = total.astype(to.dtype)

        add(2, 0, sbuf, 0)
        go(FAR_A, t)
        add(2, 1, sbuf, 2)
        go(FAR_B, t)
        add(1, 1, sbuf, 1)
        go(NEAR_B, t)
        add(3, 0, sbuf, 3)
        go(NEAR_A, t)
        add(1, 0, sf, 2)
        add(3, 1, sf, 3)
        add(0, 0, sf, 0)
        add(0, 1, sf, 1)

    def carry_on(t):
        par = lax.rem(t, 2)
        for kind, k, mine, out in ((FAR_A, 0, 2, RUN_A), (FAR_B, 2, 3, RUN_B)):
            arrived(kind, t)

            @pl.loop(0, half // 16)
            def _(i):
                here = pl.ds(i * 16, 16)
                for c in range(0, d, chunk):
                    total = rsr[par, k, here, c : c + chunk].astype(F32) + sf[mine, here, c : c + chunk]
                    rsr[par, k, here, c : c + chunk] = total.astype(BF16)

            go(out, t)

    def finish(t):
        par, s = lax.rem(t, 2), lax.rem(t, n_seq)

        @pl.when(t < n_seq)
        def _():
            row_copy(s).wait()

        @pl.when(t >= 2)
        def _():
            for kind in (RIGHT, LEFT, SIDE):
                gone(kind, t - 2)

        for kind in (NEAR_A, NEAR_B, RUN_A, RUN_B):
            arrived(kind, t)
        for part, (run, near) in enumerate(((4, 3), (5, 1))):
            @pl.loop(0, half // 16)
            def _(i):
                src, dst = pl.ds(i * 16, 16), pl.ds(part * half + i * 16, 16)
                squares = jnp.zeros((16, chunk), F32)
                for c in range(0, d, chunk):
                    cols = slice(c, c + chunk)
                    total = sf[part, src, cols] + rsr[par, run, src, cols].astype(F32) + rsr[par, near, src, cols].astype(F32)
                    h = (hrow[s, dst, cols].astype(F32) + total).astype(BF16)
                    hrow[s, dst, cols] = h
                    squares += h.astype(F32) * h.astype(F32)
                scale = lax.rsqrt(jnp.sum(squares, -1, keepdims=True) / d + EPS)
                for c in range(0, d, chunk):
                    cols = slice(c, c + chunk)
                    h = hrow[s, dst, cols].astype(F32)
                    stage[par, dst, cols] = jnp.where(t < n_seq, h * scale * gain_m[:, cols], h).astype(BF16)
        for kind in (RUN_A, RUN_B):
            gone(kind, t)
        for kind in (RIGHT, LEFT, SIDE):
            go(kind, t)
        mine_copy(t).start()

    def pass_on(t):
        for kind in (RIGHT, LEFT):
            arrived(kind, t)
        for kind in (FWD_A, FWD_B, SIDE_L, SIDE_R):
            go(kind, t)
        arrived(SIDE, t)

    def pass_last(t):
        for kind in (FWD_A, FWD_B):
            arrived(kind, t)
        go(SIDE_2, t)
        mine_copy(t).wait()

    def complete(t):
        for kind in (SIDE_L, SIDE_R, SIDE_2):
            arrived(kind, t)
        for kind in (FWD_A, FWD_B, SIDE_L, SIDE_R, SIDE_2):
            gone(kind, t)

    def back(w, lhs):
        @pl.loop(0, n_out)
        def _(n):
            slot = lax.rem(n, 2)
            out_tile(w, n).wait()
            out = _dot(lhs(), dbuf[slot, : w.shape[0], :])
            cols = pl.ds(pl.multiple_of(n * OUT, OUT), OUT)
            own[:, cols] = out[:split]
            oth[:, cols] = out[split:].astype(BF16)

            @pl.when(n + 2 < n_out)
            def _():
                out_tile(w, n + 2).start()

    def norm_rows():
        @pl.loop(0, tokens // 16)
        def _(i):
            here = pl.ds(pl.multiple_of(i * 16, 16), 16)
            squares = jnp.zeros((16, chunk), F32)
            for c in range(0, d, chunk):
                v = xb[here, c : c + chunk].astype(F32)
                squares += v * v
            scale = lax.rsqrt(jnp.sum(squares, -1, keepdims=True) / d + EPS)
            for c in range(0, d, chunk):
                cols = slice(c, c + chunk)
                xb[here, cols] = (xb[here, cols].astype(F32) * scale * gain_a[:, cols]).astype(BF16)

    def turned(t):
        return t * cos_ref[...] + pltpu.roll(t, HEAD // 2, 1) * sin_ref[...]

    def project():
        @pl.loop(0, n_wide)
        def _(n):
            on_qkv(n, wait)
            got = _dot(xb[...], wbuf[lax.rem(n, 2)]).astype(BF16).astype(F32)

            @pl.when(n + 2 < n_wide)
            def _():
                on_qkv(n + 2, start)

            first, second = got[:, :HEAD], got[:, HEAD:]
            cols = pl.multiple_of(n * WIDE, WIDE)
            hid[:, pl.ds(cols, HEAD)] = turned(first).astype(BF16)
            hid[:, pl.ds(pl.multiple_of(cols + HEAD, HEAD), HEAD)] = jnp.where(n < n_wide - 1, turned(second), second).astype(BF16)

    def attention():
        block = tokens // 2
        ahead = lax.broadcasted_iota(jnp.int32, (block, block), 1) > lax.broadcasted_iota(jnp.int32, (block, block), 0)

        @pl.loop(0, heads)
        def _(n):
            cols = pl.ds(pl.multiple_of(n * HEAD, HEAD), HEAD)
            to = pl.ds(pl.multiple_of(seen_at + n * HEAD, HEAD), HEAD)
            for i in range(2):
                q = hid[i * block : (i + 1) * block, cols]
                keys = (i + 1) * block
                scores = lax.dot_general(q, hid[:keys, k_at : k_at + HEAD], (((1,), (1,)), ((), ())), preferred_element_type=F32) * HEAD**-0.5
                last = jnp.where(ahead, -1e30, scores[:, keys - block :])
                scores = last if i == 0 else jnp.concatenate([scores[:, : keys - block], last], 1)
                weights = jnp.exp(scores - jnp.max(scores, -1, keepdims=True))
                total = jnp.sum(weights, -1, keepdims=True)
                seen = (_dot(weights.astype(BF16), hid[:keys, v_at : v_at + HEAD]) / total).astype(BF16)
                for j in range(block // rows):
                    chip, whose = divmod(i * (block // rows) + j, 2)
                    row = pl.multiple_of(lax.rem(whose + core, 2) * split + chip * rows, rows)
                    hid[pl.ds(row, rows), to] = seen[j * rows : (j + 1) * rows]

    x_copy(0).start()
    for s in range(n_seq):
        row_copy(s).start()
    barrier = pltpu.get_barrier_semaphore()
    for peer in (right, left, other):
        pl.semaphore_signal(barrier, inc=1, device_id=peer, device_id_type=MESH)
    pl.semaphore_wait(barrier, 3)

    @pl.loop(0, n_seq)
    def _(s):
        t = s - 1
        for n in range(2):
            on_qkv(jnp.int32(n), start)
            out_tile(wo, jnp.int32(n)).start()

        @pl.when(t >= 1)
        def _():
            finish(t - 1)

        @pl.when(t >= 0)
        def _():
            spread(t)

        x_copy(s).wait()
        norm_rows()
        project()

        @pl.when(s + 1 < n_seq)
        def _():
            x_copy(s + 1).start()

        @pl.when(t >= 2)
        def _():
            pass_last(t - 2)

        @pl.when(t >= 1)
        def _():
            pass_on(t - 1)

        @pl.when(t >= 0)
        def _():
            carry_on(t)

        attention()
        back(wo, lambda: hid[:, seen_at : seen_at + qw])
        go(D2D, s)

    @pl.loop(0, n_seq)
    def _(m):
        t = m + n_seq - 1
        tile(w_gate, jnp.int32(0), 0).start()
        tile(w_up, jnp.int32(0), 1).start()
        for n in range(2):
            out_tile(w_down, jnp.int32(n)).start()
        complete(m)
        for copy in b_copies(m):
            copy.start()
        finish(t - 1)
        spread(t)
        for copy in b_copies(m):
            copy.wait()

        @pl.loop(0, n_ff)
        def _(i):
            tile(w_gate, i, 0).wait()
            gate_s[...] = _dot(xb[...], wbuf[0])

            @pl.when(i + 1 < n_ff)
            def _():
                tile(w_gate, i + 1, 0).start()

            tile(w_up, i, 1).wait()
            up = _dot(xb[...], wbuf[1])
            hid[:, pl.ds(pl.multiple_of(i * WIDE, WIDE), WIDE)] = (jax.nn.silu(gate_s[...]) * up).astype(BF16)

            @pl.when(i + 1 < n_ff)
            def _():
                tile(w_up, i + 1, 1).start()

            @pl.when(i == n_ff // 2)
            def _():
                pass_last(t - 2)
                pass_on(t - 1)

            @pl.when(i == n_ff - 2)
            def _():
                carry_on(t)

        back(w_down, lambda: hid[...])
        go(D2D, t + 1)

    last = jnp.int32(2 * n_seq - 1)
    finish(last - 1)
    spread(last)
    pass_last(last - 2)
    pass_on(last - 1)
    carry_on(last)
    finish(last)
    pass_last(last - 1)
    pass_on(last)
    pass_last(last)

    @pl.loop(n_seq, 2 * n_seq)
    def _(t):
        complete(t)

    for kind in (FAR_A, NEAR_B, FAR_B, NEAR_A):
        gone(kind, last)
    for t in (last - 1, last):
        for kind in (RIGHT, LEFT, SIDE):
            gone(kind, t)


def solution(mesh):
    tp = mesh.shape["tp"]
    chips = tp // 2
    assert chips == 4

    def step(x, gain_a, wq, wk, wv, wo, gain_m, w_gate, w_up, w_down):
        n_seq, tokens, d = x.shape
        rows = tokens // tp
        ff = w_down.shape[0]
        angle = jnp.arange(tokens, dtype=F32)[:, None] * THETA ** (-jnp.arange(HEAD // 2, dtype=F32) / (HEAD // 2))
        cos, sin = jnp.cos(angle), jnp.sin(angle)
        cos, sin = jnp.concatenate([cos, cos], 1), jnp.concatenate([-sin, sin], 1)
        gains = [g.astype(F32).reshape(1, d) for g in (gain_a, gain_m)]
        vmem, hbm = pl.BlockSpec(memory_space=pltpu.VMEM), pl.BlockSpec(memory_space=pl.ANY)
        half = rows // 2
        dma = pltpu.SemaphoreType.DMA
        out = pl.pallas_call(
            _layer,
            out_shape=jax.ShapeDtypeStruct((2 * n_seq, chips, 2, rows, d), BF16),
            in_specs=[hbm, vmem, vmem, vmem, vmem] + [hbm] * 7,
            out_specs=hbm,
            scratch_shapes=[
                pltpu.VMEM((tokens, d), BF16),
                pltpu.VMEM((2, d, WIDE), BF16),
                pltpu.VMEM((2, ff, OUT), BF16),
                pltpu.VMEM((tokens // 2, d), F32),
                pltpu.VMEM((tokens // 2, d), BF16),
                pltpu.VMEM((2, tokens // 2, d), BF16),
                pltpu.VMEM((tokens, ff), BF16),
                pltpu.VMEM((tokens, WIDE), F32),
                pltpu.VMEM((2, 6, half, d), BF16),
                pltpu.VMEM((4, half, d), BF16),
                pltpu.VMEM((4, half, d), F32),
                pltpu.VMEM((n_seq, rows, d), BF16),
                pltpu.VMEM((2, rows, d), BF16),
                dma((15, 2 * n_seq)), dma((15, 2 * n_seq)),
                dma((2 * chips + 1,)), dma((2,)), dma((2,)), dma((2,)), dma((n_seq,)), dma((2 * n_seq,)),
            ],
            compiler_params=pltpu.CompilerParams(collective_id=0, has_side_effects=True, vmem_limit_bytes=62 * 2**20),
        )(x, *gains, cos, sin, wq, wk, wv, wo, w_gate, w_up, w_down)
        return out[n_seq:].reshape(x.shape)

    tokens, whole, columns, rows_of = P("dp", None, None), P(None), P(None, "tp"), P("tp", None)
    return jax.shard_map(
        step,
        mesh=mesh,
        in_specs=(tokens, whole, columns, columns, columns, rows_of, whole, columns, columns, rows_of),
        out_specs=tokens,
        check_vma=False,
    )
```

```python
import functools

import jax
import jax.numpy as jnp
import numpy as np
from jax import lax
from jax.experimental import pallas as pl
from jax.experimental.pallas import tpu as pltpu
from jax.sharding import PartitionSpec as P

HEAD = 128
THETA = 10000
EPS = 1e-6
WIDE = 512
OUT = 1024
BF16, F32 = jnp.bfloat16, jnp.float32
MESH = pl.DeviceIdType.MESH
D2D, FAR_A, NEAR_B, FAR_B, NEAR_A, RUN_A, RUN_B, RIGHT, LEFT, SIDE, FWD_A, FWD_B, SIDE_L, SIDE_R, SIDE_2 = range(15)
KINDS = 17


def _dot(a, b):
    return jnp.dot(a, b, preferred_element_type=F32)


def _layer(x_ref, gains, cos_ref, sin_ref, wq, wk, wv, wo, w_gate, w_up, w_down, g_ref,
           xb, wbuf, dbuf, own, oth, sib, hid, rsr, sbuf, sf, hrow, stage,
           send, recv, xsem, wsem, vsem, dsem, hsem, lsem):
    n_seq, tokens, d = x_ref.shape
    chips, rows = g_ref.shape[1], g_ref.shape[3]
    half = rows // 2
    split = chips * rows
    qw, ff = wq.shape[1], w_down.shape[0]
    heads = qw // HEAD
    k_at, v_at, seen_at = qw, qw + HEAD, qw + 2 * HEAD
    n_wide, n_out = (qw + 2 * HEAD) // WIDE, d // OUT
    part = WIDE // 2
    n_ff = ff // part
    cuts = sorted({n_out // 2, n_out * 5 // 6, n_out})
    pieces = list(zip((D2D, 15, 16), [0, *cuts], cuts))
    chunk = d // 4

    at = lax.axis_index("tp")
    me, core = at // 2, lax.rem(at, 2)
    rel = lambda k: lax.rem(me + k, chips)
    device = lambda chip: {"tp": chip * 2 + core}
    right, left, other = device(rel(1)), device(rel(chips - 1)), {"tp": me * 2 + 1 - core}

    def x_copy(s):
        return pltpu.make_async_copy(x_ref.at[s], xb, xsem.at[2 * chips])

    def b_copies(m):
        return [pltpu.make_async_copy(g_ref.at[m, k, core if j == 0 else 1 - core], xb.at[pl.ds(j * split + k * rows, rows)],
                                      xsem.at[j * chips + k]) for j in range(2) for k in range(chips)]

    def row_copy(s):
        return pltpu.make_async_copy(x_ref.at[s, pl.ds(pl.multiple_of(at * rows, rows), rows)], hrow.at[s], hsem.at[s])

    def pair(n):
        slot, cols = lax.rem(n, 2), pl.ds(pl.multiple_of(n * part, part), part)
        return [pltpu.make_async_copy(w.at[:, cols], wbuf.at[slot, :, pl.ds(j * part, part)], wsem.at[slot, j])
                for j, w in enumerate((w_gate, w_up))]

    def on_pair(n, act):
        for copy in pair(n):
            act(copy)

    def on_qkv(n, act):
        slot = lax.rem(n, 2)
        rest = WIDE - 2 * HEAD

        @pl.when(n < n_wide - 1)
        def _():
            act(pltpu.make_async_copy(wq.at[:, pl.ds(pl.multiple_of(n * WIDE, WIDE), WIDE)], wbuf.at[slot], wsem.at[slot, 0]))

        @pl.when(n == n_wide - 1)
        def _():
            act(pltpu.make_async_copy(wq.at[:, pl.ds(qw - rest, rest)], wbuf.at[slot, :, pl.ds(0, rest)], wsem.at[slot, 0]))
            act(pltpu.make_async_copy(wk, wbuf.at[slot, :, pl.ds(rest, HEAD)], wsem.at[slot, 1]))
            act(pltpu.make_async_copy(wv, wbuf.at[slot, :, pl.ds(rest + HEAD, HEAD)], vsem.at[0]))

    def out_tile(w, n):
        slot = lax.rem(n, 2)
        return pltpu.make_async_copy(w.at[:, pl.ds(pl.multiple_of(n * OUT, OUT), OUT)], dbuf.at[slot, pl.ds(0, w.shape[0])], dsem.at[slot])

    start, wait = lambda copy: copy.start(), lambda copy: copy.wait()

    def message(kind, t, src, dst, to):
        return pltpu.make_async_remote_copy(src_ref=src, dst_ref=dst, send_sem=send.at[kind, t], recv_sem=recv.at[kind, t],
                                            device_id=to, device_id_type=MESH)

    def sent(kind, t):
        par = lax.rem(t, 2)
        part_a, part_b = pl.ds(0, half), pl.ds(half, half)
        for piece, a, b in pieces:
            if kind == piece:
                cols = pl.ds(a * OUT, (b - a) * OUT)
                return message(kind, t, oth.at[:, cols], sib.at[par, :, cols], other)
        if kind in (FAR_A, NEAR_B, FAR_B, NEAR_A):
            k = kind - FAR_A
            return message(kind, t, sbuf.at[k], rsr.at[par, k], right if k < 2 else left)
        if kind == RUN_A:
            return message(kind, t, rsr.at[par, 0], rsr.at[par, 4], right)
        if kind == RUN_B:
            return message(kind, t, rsr.at[par, 2], rsr.at[par, 5], left)
        mine = g_ref.at[t, me, core]
        if kind in (RIGHT, LEFT, SIDE):
            return message(kind, t, stage.at[par], mine, {RIGHT: right, LEFT: left, SIDE: other}[kind])
        if kind == FWD_A:
            ref = g_ref.at[t, rel(chips - 1), core, part_a]
            return message(kind, t, ref, ref, right)
        if kind == FWD_B:
            ref = g_ref.at[t, rel(1), core, part_b]
            return message(kind, t, ref, ref, left)
        ref = g_ref.at[t, rel({SIDE_L: chips - 1, SIDE_R: 1, SIDE_2: 2}[kind]), core]
        return message(kind, t, ref, ref, other)

    def arrived(kind, t):
        par = lax.rem(t, 2)
        part_a, part_b = pl.ds(0, half), pl.ds(half, half)
        cols = [pl.ds(a * OUT, (b - a) * OUT) for piece, a, b in pieces if kind == piece]
        if cols:
            ref, who = sib.at[par, :, cols[0]], other
        elif kind in (FAR_A, NEAR_B, FAR_B, NEAR_A):
            k = kind - FAR_A
            ref, who = rsr.at[par, k], (left if k < 2 else right)
        elif kind == RUN_A:
            ref, who = rsr.at[par, 4], left
        elif kind == RUN_B:
            ref, who = rsr.at[par, 5], right
        elif kind == RIGHT:
            ref, who = g_ref.at[t, rel(chips - 1), core], left
        elif kind == LEFT:
            ref, who = g_ref.at[t, rel(1), core], right
        elif kind == FWD_A:
            ref, who = g_ref.at[t, rel(2), core, part_a], left
        elif kind == FWD_B:
            ref, who = g_ref.at[t, rel(2), core, part_b], right
        else:
            ref, who = g_ref.at[t, rel({SIDE: 0, SIDE_L: chips - 1, SIDE_R: 1, SIDE_2: 2}[kind]), 1 - core], other
        message(kind, t, ref, ref, who).wait_recv()

    def go(kind, t):
        sent(kind, t).start()

    def gone(kind, t):
        sent(kind, t).wait_send()

    def mine_copy(t):
        return pltpu.make_async_copy(stage.at[lax.rem(t, 2)], g_ref.at[t, me, core], lsem.at[t])

    def add(t, k, piece, to, slot):
        par, base = lax.rem(t, 2), rel(k) * rows + piece * half

        @pl.loop(0, half // 16)
        def _(i):
            here = pl.ds(pl.multiple_of(base + i * 16, 16), 16)
            for c in range(0, d, chunk):
                total = own[here, c : c + chunk] + sib[par, here, c : c + chunk].astype(F32)
                to[slot, pl.ds(i * 16, 16), c : c + chunk] = total.astype(to.dtype)

    def spread_far(t):
        for piece, _, _ in pieces:
            gone(piece, t)
            arrived(piece, t)

        @pl.when(t >= 1)
        def _():
            for kind in (FAR_A, NEAR_B, FAR_B, NEAR_A):
                gone(kind, t - 1)

        add(t, 2, 0, sbuf, 0)
        go(FAR_A, t)
        add(t, 2, 1, sbuf, 2)
        go(FAR_B, t)

    def spread_near(t):
        add(t, 1, 1, sbuf, 1)
        go(NEAR_B, t)
        add(t, 3, 0, sbuf, 3)
        go(NEAR_A, t)
        add(t, 1, 0, sf, 2)
        add(t, 3, 1, sf, 3)
        add(t, 0, 0, sf, 0)
        add(t, 0, 1, sf, 1)

    def carry_on(t):
        par = lax.rem(t, 2)
        for kind, k, mine, out in ((FAR_A, 0, 2, RUN_A), (FAR_B, 2, 3, RUN_B)):
            arrived(kind, t)

            @pl.loop(0, half // 16)
            def _(i):
                here = pl.ds(i * 16, 16)
                for c in range(0, d, chunk):
                    total = rsr[par, k, here, c : c + chunk].astype(F32) + sf[mine, here, c : c + chunk]
                    rsr[par, k, here, c : c + chunk] = total.astype(BF16)

            go(out, t)

    def finish(t):
        par, s = lax.rem(t, 2), lax.rem(t, n_seq)

        @pl.when(t < n_seq)
        def _():
            row_copy(s).wait()

        @pl.when(t >= 2)
        def _():
            for kind in (RIGHT, LEFT, SIDE):
                gone(kind, t - 2)

        for kind in (NEAR_A, NEAR_B, RUN_A, RUN_B):
            arrived(kind, t)
        for part, (run, near) in enumerate(((4, 3), (5, 1))):
            @pl.loop(0, half // 16)
            def _(i):
                src, dst = pl.ds(i * 16, 16), pl.ds(part * half + i * 16, 16)
                squares = jnp.zeros((16, chunk), F32)
                for c in range(0, d, chunk):
                    cols = slice(c, c + chunk)
                    total = sf[part, src, cols] + rsr[par, run, src, cols].astype(F32) + rsr[par, near, src, cols].astype(F32)
                    h = (hrow[s, dst, cols].astype(F32) + total).astype(BF16)
                    hrow[s, dst, cols] = h
                    squares += h.astype(F32) * h.astype(F32)
                scale = lax.rsqrt(jnp.sum(squares, -1, keepdims=True) / d + EPS)
                for c in range(0, d, chunk):
                    cols = slice(c, c + chunk)
                    h = hrow[s, dst, cols].astype(F32)
                    stage[par, dst, cols] = jnp.where(t < n_seq, h * scale * gains[1:2, cols], h).astype(BF16)
        for kind in (RUN_A, RUN_B):
            gone(kind, t)
        for kind in (RIGHT, LEFT, SIDE):
            go(kind, t)
        mine_copy(t).start()

    def pass_on(t):
        for kind in (RIGHT, LEFT):
            arrived(kind, t)
        for kind in (FWD_A, FWD_B, SIDE_L, SIDE_R):
            go(kind, t)

    def pass_last(t):
        for kind in (FWD_A, FWD_B):
            arrived(kind, t)
        go(SIDE_2, t)
        mine_copy(t).wait()

    def complete(t):
        for kind in (SIDE_L, SIDE_R, SIDE_2):
            arrived(kind, t)
        for kind in (FWD_A, FWD_B, SIDE_L, SIDE_R, SIDE_2):
            gone(kind, t)

    def back(w, lhs, t, hooks=()):
        @pl.loop(0, n_out)
        def _(n):
            slot = lax.rem(n, 2)
            out_tile(w, n).wait()
            out = _dot(lhs(), dbuf[slot, : w.shape[0], :])
            cols = pl.ds(pl.multiple_of(n * OUT, OUT), OUT)
            own[:, cols] = out[:split]
            oth[:, cols] = out[split:].astype(BF16)
            for piece, _, b in pieces:
                @pl.when(n == b - 1)
                def _():
                    go(piece, t)

            for k, hook in enumerate(hooks):
                @pl.when(n == min(2 * k, n_out - 1))
                def _():
                    hook()

            @pl.when(n + 2 < n_out)
            def _():
                out_tile(w, n + 2).start()

    def norm_rows():
        narrow = d // 8

        @pl.loop(0, tokens // 32)
        def _(i):
            here = pl.ds(pl.multiple_of(i * 32, 32), 32)
            squares = jnp.zeros((32, narrow), F32)
            for c in range(0, d, narrow):
                v = xb[here, c : c + narrow].astype(F32)
                squares += v * v
            scale = lax.rsqrt(jnp.sum(squares, -1, keepdims=True) / d + EPS)
            for c in range(0, d, narrow):
                cols = slice(c, c + narrow)
                xb[here, cols] = (xb[here, cols].astype(F32) * scale * gains[0:1, cols]).astype(BF16)

    def turned(t):
        return t * cos_ref[...] + pltpu.roll(t, HEAD // 2, 1) * sin_ref[...]

    def project():
        @pl.loop(0, n_wide)
        def _(n):
            on_qkv(n, wait)
            got = _dot(xb[...], wbuf[lax.rem(n, 2)]).astype(BF16).astype(F32)

            @pl.when(n + 2 < n_wide)
            def _():
                on_qkv(n + 2, start)

            for j in range(WIDE // HEAD):
                t = got[:, j * HEAD : (j + 1) * HEAD]
                value = turned(t) if j < WIDE // HEAD - 1 else jnp.where(n < n_wide - 1, turned(t), t)
                hid[:, pl.ds(pl.multiple_of(n * WIDE + j * HEAD, HEAD), HEAD)] = value.astype(BF16)

    def attention():
        block = tokens // 2
        ahead = lax.broadcasted_iota(jnp.int32, (block, block), 1) > lax.broadcasted_iota(jnp.int32, (block, block), 0)

        @pl.loop(0, heads)
        def _(n):
            cols = pl.ds(pl.multiple_of(n * HEAD, HEAD), HEAD)
            to = pl.ds(pl.multiple_of(seen_at + n * HEAD, HEAD), HEAD)
            for i in range(2):
                q = hid[i * block : (i + 1) * block, cols]
                keys = (i + 1) * block
                scores = lax.dot_general(q, hid[:keys, k_at : k_at + HEAD], (((1,), (1,)), ((), ())), preferred_element_type=F32) * HEAD**-0.5
                last = jnp.where(ahead, -1e30, scores[:, keys - block :])
                scores = last if i == 0 else jnp.concatenate([scores[:, : keys - block], last], 1)
                weights = jnp.exp(scores - jnp.max(scores, -1, keepdims=True))
                total = jnp.sum(weights, -1, keepdims=True)
                seen = (_dot(weights.astype(BF16), hid[:keys, v_at : v_at + HEAD]) / total).astype(BF16)
                for j in range(block // rows):
                    chip, whose = divmod(i * (block // rows) + j, 2)
                    row = pl.multiple_of(lax.rem(whose + core, 2) * split + chip * rows, rows)
                    hid[pl.ds(row, rows), to] = seen[j * rows : (j + 1) * rows]

    x_copy(0).start()
    for s in range(n_seq):
        row_copy(s).start()
    barrier = pltpu.get_barrier_semaphore()
    for peer in (right, left, other):
        pl.semaphore_signal(barrier, inc=1, device_id=peer, device_id_type=MESH)
    pl.semaphore_wait(barrier, 3)

    @pl.loop(0, n_seq)
    def _(s):
        t = s - 1
        @pl.when(t >= 0)
        def _():
            spread_far(t)

        @pl.when(t >= 1)
        def _():
            finish(t - 1)

        @pl.when(t >= 0)
        def _():
            spread_near(t)

        x_copy(s).wait()

        @pl.when(s == 0)
        def _():
            for n in range(min(2, n_wide)):
                on_qkv(jnp.int32(n), start)

        norm_rows()
        for n in range(2):
            out_tile(wo, jnp.int32(n)).start()
        project()

        @pl.when(s + 1 < n_seq)
        def _():
            x_copy(s + 1).start()
            for n in range(min(2, n_wide)):
                on_qkv(jnp.int32(n), start)

        @pl.when(s + 1 == n_seq)
        def _():
            for n in range(2):
                on_pair(jnp.int32(n), start)

        @pl.when(t >= 0)
        def _():
            carry_on(t)

        attention()

        @pl.when(t >= 1)
        def _():
            arrived(SIDE, t - 1)

        back(wo, lambda: hid[:, seen_at : seen_at + qw], s)

        @pl.when(t >= 1)
        def _():
            pass_on(t - 1)

        @pl.when(t >= 2)
        def _():
            pass_last(t - 2)

    def load(m):
        complete(m)
        for copy in b_copies(m):
            copy.start()

    @pl.loop(0, n_seq)
    def _(m):
        t = m + n_seq - 1
        for n in range(2):
            out_tile(w_down, jnp.int32(n)).start()

        @pl.when(m == 0)
        def _():
            load(0)

        spread_far(t)
        finish(t - 1)
        spread_near(t)
        for copy in b_copies(m):
            copy.wait()

        @pl.loop(0, n_ff)
        def _(i):
            on_pair(i, wait)
            both = _dot(xb[...], wbuf[lax.rem(i, 2)])
            hid[:, pl.ds(pl.multiple_of(i * part, part), part)] = (jax.nn.silu(both[:, :part]) * both[:, part:]).astype(BF16)

            @pl.when(i + 2 < n_ff)
            def _():
                on_pair(i + 2, start)

            @pl.when(i == n_ff // 4)
            def _():
                carry_on(t)

            @pl.when(i == n_ff - 2)
            def _():
                pass_on(t - 1)
                pass_last(t - 2)

        arrived(SIDE, t - 1)

        def ahead(act):
            @pl.when(m + 1 < n_seq)
            def _():
                act()

        back(w_down, lambda: hid[...], t + 1, [lambda: ahead(lambda: on_pair(jnp.int32(0), start)), lambda: ahead(lambda: load(m + 1)),
                                               lambda: ahead(lambda: on_pair(jnp.int32(1), start))])

    last = jnp.int32(2 * n_seq - 1)
    spread_far(last)
    finish(last - 1)
    spread_near(last)
    carry_on(last)
    arrived(SIDE, last - 1)
    pass_on(last - 1)
    pass_last(last - 2)
    finish(last)
    pass_last(last - 1)
    arrived(SIDE, last)
    pass_on(last)
    pass_last(last)

    @pl.loop(n_seq, 2 * n_seq)
    def _(t):
        complete(t)

    for kind in (FAR_A, NEAR_B, FAR_B, NEAR_A):
        gone(kind, last)
    for t in (last - 1, last):
        for kind in (RIGHT, LEFT, SIDE):
            gone(kind, t)


def _taken(g):
    _, n_seq, tokens, d = g.shape
    cut = 4
    rows = tokens // cut
    places = [(i, pl.ds(j * rows, rows)) for i in range(n_seq) for j in range(cut)]

    def body(src, dst, held, taken, put):
        reads = [pltpu.make_async_copy(src.at[1, i, at], held.at[i, at], taken.at[k]) for k, (i, at) in enumerate(places)]
        writes = [pltpu.make_async_copy(held.at[i, at], dst.at[i, at], put.at[k]) for k, (i, at) in enumerate(places)]
        for read in reads:
            read.start()
        for read, write in zip(reads, writes):
            read.wait()
            write.start()
        for write in writes:
            write.wait()

    hbm = pl.BlockSpec(memory_space=pl.ANY)
    return pl.pallas_call(
        body,
        out_shape=jax.ShapeDtypeStruct((n_seq, tokens, d), g.dtype),
        in_specs=[hbm],
        out_specs=hbm,
        scratch_shapes=[pltpu.VMEM((n_seq, tokens, d), g.dtype), pltpu.SemaphoreType.DMA((len(places),)), pltpu.SemaphoreType.DMA((len(places),))],
        compiler_params=pltpu.CompilerParams(vmem_limit_bytes=60 * 2**20),
    )(g)


def solution(mesh):
    tp = mesh.shape["tp"]
    chips = tp // 2
    assert chips == 4

    def step(x, gain_a, wq, wk, wv, wo, gain_m, w_gate, w_up, w_down):
        n_seq, tokens, d = x.shape
        rows = tokens // tp
        ff = w_down.shape[0]
        angle = np.arange(tokens, dtype=np.float32)[:, None] * np.float32(THETA) ** (-np.arange(HEAD // 2, dtype=np.float32) / (HEAD // 2))
        cos, sin = np.cos(angle), np.sin(angle)
        cos, sin = jnp.asarray(np.concatenate([cos, cos], 1)), jnp.asarray(np.concatenate([-sin, sin], 1))
        gains = jnp.stack([gain_a, gain_m]).astype(F32)
        vmem, hbm = pl.BlockSpec(memory_space=pltpu.VMEM), pl.BlockSpec(memory_space=pl.ANY)
        half = rows // 2
        dma = pltpu.SemaphoreType.DMA
        out = pl.pallas_call(
            _layer,
            out_shape=jax.ShapeDtypeStruct((2 * n_seq, chips, 2, rows, d), BF16),
            in_specs=[hbm, vmem, vmem, vmem] + [hbm] * 7,
            out_specs=hbm,
            scratch_shapes=[
                pltpu.VMEM((tokens, d), BF16),
                pltpu.VMEM((2, d, WIDE), BF16),
                pltpu.VMEM((2, ff, OUT), BF16),
                pltpu.VMEM((tokens // 2, d), F32),
                pltpu.VMEM((tokens // 2, d), BF16),
                pltpu.VMEM((2, tokens // 2, d), BF16),
                pltpu.VMEM((tokens, ff), BF16),
                pltpu.VMEM((2, 6, half, d), BF16),
                pltpu.VMEM((4, half, d), BF16),
                pltpu.VMEM((4, half, d), F32),
                pltpu.VMEM((n_seq, rows, d), BF16),
                pltpu.VMEM((2, rows, d), BF16),
                dma((KINDS, 2 * n_seq)), dma((KINDS, 2 * n_seq)),
                dma((2 * chips + 1,)), dma((2, 2)), dma((1,)), dma((2,)), dma((n_seq,)), dma((2 * n_seq,)),
            ],
            compiler_params=pltpu.CompilerParams(collective_id=0, has_side_effects=True, vmem_limit_bytes=62 * 2**20),
        )(x, gains, cos, sin, wq, wk, wv, wo, w_gate, w_up, w_down)
        return _taken(out.reshape(2, n_seq, tokens, d))

    tokens, whole, columns, rows_of = P("dp", None, None), P(None), P(None, "tp"), P("tp", None)
    return jax.shard_map(
        step,
        mesh=mesh,
        in_specs=(tokens, whole, columns, columns, columns, rows_of, whole, columns, columns, rows_of),
        out_specs=tokens,
        check_vma=False,
    )
```

```python
import functools

import jax
import jax.numpy as jnp
import numpy as np
from jax import lax
from jax.experimental import pallas as pl
from jax.experimental.pallas import tpu as pltpu
from jax.sharding import PartitionSpec as P

HEAD = 128
THETA = 10000
EPS = 1e-6
WIDE = 512
OUT = 1024
BF16, F32 = jnp.bfloat16, jnp.float32
MESH = pl.DeviceIdType.MESH
D2D, FAR_A, NEAR_B, FAR_B, NEAR_A, RUN_A, RUN_B, RIGHT, LEFT, SIDE, FWD_A, FWD_B, SIDE_L, SIDE_R, SIDE_2 = range(15)
KINDS = 19
RIGHT_2, LEFT_2 = 17, 18


def _dot(a, b):
    return jnp.dot(a, b, preferred_element_type=F32)


def _layer(x_ref, gains, cos_ref, sin_ref, wq, wk, wv, wo, w_gate, w_up, w_down, g_ref,
           xb, wbuf, dbuf, own, oth, sib, hid, seen_s, rsr, sbuf, sf, hrow, stage,
           send, recv, xsem, wsem, vsem, dsem, hsem, lsem):
    n_seq, tokens, d = x_ref.shape
    chips, rows = g_ref.shape[1], g_ref.shape[3]
    half = rows // 2
    split = chips * rows
    qw, ff = wq.shape[1], w_down.shape[0]
    heads = qw // HEAD
    k_at, v_at = qw, qw + HEAD
    n_wide, n_out = (qw + 2 * HEAD) // WIDE, d // OUT
    part = WIDE // 2
    n_ff = ff // part
    cuts = sorted({n_out // 2, n_out * 5 // 6, n_out})
    pieces = list(zip((D2D, 15, 16), [0, *cuts], cuts))
    chunk = d // 4

    at = lax.axis_index("tp")
    me, core = at // 2, lax.rem(at, 2)
    rel = lambda k: lax.rem(me + k, chips)
    device = lambda chip: {"tp": chip * 2 + core}
    right, left, other = device(rel(1)), device(rel(chips - 1)), {"tp": me * 2 + 1 - core}

    def x_copy(s):
        return pltpu.make_async_copy(x_ref.at[s], xb, xsem.at[2 * chips])

    def b_copies(m):
        return [pltpu.make_async_copy(g_ref.at[m, k, core if j == 0 else 1 - core], xb.at[pl.ds(j * split + k * rows, rows)],
                                      xsem.at[j * chips + k]) for j in range(2) for k in range(chips)]

    def row_copy(s):
        return pltpu.make_async_copy(x_ref.at[s, pl.ds(pl.multiple_of(at * rows, rows), rows)], hrow.at[s], hsem.at[s])

    def pair(n):
        slot, cols = lax.rem(n, 2), pl.ds(pl.multiple_of(n * part, part), part)
        return [pltpu.make_async_copy(w.at[:, cols], wbuf.at[slot, :, pl.ds(j * part, part)], wsem.at[slot, j])
                for j, w in enumerate((w_gate, w_up))]

    def on_pair(n, act):
        for copy in pair(n):
            act(copy)

    def on_qkv(n, act):
        slot = lax.rem(n, 2)
        rest = WIDE - 2 * HEAD

        @pl.when(n < n_wide - 1)
        def _():
            act(pltpu.make_async_copy(wq.at[:, pl.ds(pl.multiple_of(n * WIDE, WIDE), WIDE)], wbuf.at[slot], wsem.at[slot, 0]))

        @pl.when(n == n_wide - 1)
        def _():
            act(pltpu.make_async_copy(wq.at[:, pl.ds(qw - rest, rest)], wbuf.at[slot, :, pl.ds(0, rest)], wsem.at[slot, 0]))
            act(pltpu.make_async_copy(wk, wbuf.at[slot, :, pl.ds(rest, HEAD)], wsem.at[slot, 1]))
            act(pltpu.make_async_copy(wv, wbuf.at[slot, :, pl.ds(rest + HEAD, HEAD)], vsem.at[0]))

    def out_tile(w, n):
        slot = lax.rem(n, 2)
        return pltpu.make_async_copy(w.at[:, pl.ds(pl.multiple_of(n * OUT, OUT), OUT)], dbuf.at[slot, pl.ds(0, w.shape[0])], dsem.at[slot])

    start, wait = lambda copy: copy.start(), lambda copy: copy.wait()

    def message(kind, t, src, dst, to):
        return pltpu.make_async_remote_copy(src_ref=src, dst_ref=dst, send_sem=send.at[kind, t], recv_sem=recv.at[kind, t],
                                            device_id=to, device_id_type=MESH)

    def sent(kind, t):
        par = lax.rem(t, 2)
        part_a, part_b = pl.ds(0, half), pl.ds(half, half)
        for piece, a, b in pieces:
            if kind == piece:
                cols = pl.ds(a * OUT, (b - a) * OUT)
                return message(kind, t, oth.at[:, cols], sib.at[par, :, cols], other)
        if kind in (FAR_A, NEAR_B, FAR_B, NEAR_A):
            k = kind - FAR_A
            return message(kind, t, sbuf.at[k], rsr.at[par, k], right if k < 2 else left)
        if kind == RUN_A:
            return message(kind, t, rsr.at[par, 0], rsr.at[par, 4], right)
        if kind == RUN_B:
            return message(kind, t, rsr.at[par, 2], rsr.at[par, 5], left)
        mine = g_ref.at[t, me, core]
        if kind == SIDE:
            return message(kind, t, stage.at[par], mine, other)
        if kind in (RIGHT, LEFT_2):
            return message(kind, t, stage.at[par, part_a], g_ref.at[t, me, core, part_a], right if kind == RIGHT else left)
        if kind in (LEFT, RIGHT_2):
            return message(kind, t, stage.at[par, part_b], g_ref.at[t, me, core, part_b], left if kind == LEFT else right)
        if kind == FWD_A:
            ref = g_ref.at[t, rel(chips - 1), core, part_a]
            return message(kind, t, ref, ref, right)
        if kind == FWD_B:
            ref = g_ref.at[t, rel(1), core, part_b]
            return message(kind, t, ref, ref, left)
        ref = g_ref.at[t, rel({SIDE_L: chips - 1, SIDE_R: 1, SIDE_2: 2}[kind]), core]
        return message(kind, t, ref, ref, other)

    def arrived(kind, t):
        par = lax.rem(t, 2)
        part_a, part_b = pl.ds(0, half), pl.ds(half, half)
        cols = [pl.ds(a * OUT, (b - a) * OUT) for piece, a, b in pieces if kind == piece]
        if cols:
            ref, who = sib.at[par, :, cols[0]], other
        elif kind in (FAR_A, NEAR_B, FAR_B, NEAR_A):
            k = kind - FAR_A
            ref, who = rsr.at[par, k], (left if k < 2 else right)
        elif kind == RUN_A:
            ref, who = rsr.at[par, 4], left
        elif kind == RUN_B:
            ref, who = rsr.at[par, 5], right
        elif kind in (RIGHT, RIGHT_2):
            ref, who = g_ref.at[t, rel(chips - 1), core, part_a if kind == RIGHT else part_b], left
        elif kind in (LEFT, LEFT_2):
            ref, who = g_ref.at[t, rel(1), core, part_b if kind == LEFT else part_a], right
        elif kind == FWD_A:
            ref, who = g_ref.at[t, rel(2), core, part_a], left
        elif kind == FWD_B:
            ref, who = g_ref.at[t, rel(2), core, part_b], right
        else:
            ref, who = g_ref.at[t, rel({SIDE: 0, SIDE_L: chips - 1, SIDE_R: 1, SIDE_2: 2}[kind]), 1 - core], other
        message(kind, t, ref, ref, who).wait_recv()

    def go(kind, t):
        sent(kind, t).start()

    def gone(kind, t):
        sent(kind, t).wait_send()

    def mine_copy(t):
        return pltpu.make_async_copy(stage.at[lax.rem(t, 2)], g_ref.at[t, me, core], lsem.at[t])

    def add(t, k, piece, to, slot):
        par, base = lax.rem(t, 2), rel(k) * rows + piece * half

        @pl.loop(0, half // 16)
        def _(i):
            here = pl.ds(pl.multiple_of(base + i * 16, 16), 16)
            for c in range(0, d, chunk):
                total = own[here, c : c + chunk] + sib[par, here, c : c + chunk].astype(F32)
                to[slot, pl.ds(i * 16, 16), c : c + chunk] = total.astype(to.dtype)

    def spread_far(t):
        for piece, _, _ in pieces:
            gone(piece, t)
            arrived(piece, t)

        @pl.when(t >= 1)
        def _():
            for kind in (FAR_A, NEAR_B, FAR_B, NEAR_A):
                gone(kind, t - 1)

        add(t, 2, 0, sbuf, 0)
        go(FAR_A, t)
        add(t, 2, 1, sbuf, 2)
        go(FAR_B, t)

    def spread_near(t):
        add(t, 1, 1, sbuf, 1)
        go(NEAR_B, t)
        add(t, 3, 0, sbuf, 3)
        go(NEAR_A, t)
        add(t, 1, 0, sf, 2)
        add(t, 3, 1, sf, 3)
        add(t, 0, 0, sf, 0)
        add(t, 0, 1, sf, 1)

    def carry_on(t):
        par = lax.rem(t, 2)
        for kind, k, mine, out in ((FAR_A, 0, 2, RUN_A), (FAR_B, 2, 3, RUN_B)):
            arrived(kind, t)

            @pl.loop(0, half // 16)
            def _(i):
                here = pl.ds(i * 16, 16)
                for c in range(0, d, chunk):
                    total = rsr[par, k, here, c : c + chunk].astype(F32) + sf[mine, here, c : c + chunk]
                    rsr[par, k, here, c : c + chunk] = total.astype(BF16)

            go(out, t)

    def finish(t):
        par, s = lax.rem(t, 2), lax.rem(t, n_seq)

        @pl.when(t < n_seq)
        def _():
            row_copy(s).wait()

        @pl.when(t >= 2)
        def _():
            for kind in (RIGHT, LEFT, RIGHT_2, LEFT_2, SIDE):
                gone(kind, t - 2)

        for kind in (NEAR_A, NEAR_B, RUN_A, RUN_B):
            arrived(kind, t)
        for part, (run, near) in enumerate(((4, 3), (5, 1))):
            @pl.loop(0, half // 16)
            def _(i):
                src, dst = pl.ds(i * 16, 16), pl.ds(part * half + i * 16, 16)
                squares = jnp.zeros((16, chunk), F32)
                for c in range(0, d, chunk):
                    cols = slice(c, c + chunk)
                    total = sf[part, src, cols] + rsr[par, run, src, cols].astype(F32) + rsr[par, near, src, cols].astype(F32)
                    h = (hrow[s, dst, cols].astype(F32) + total).astype(BF16)
                    hrow[s, dst, cols] = h
                    squares += h.astype(F32) * h.astype(F32)
                scale = lax.rsqrt(jnp.sum(squares, -1, keepdims=True) / d + EPS)
                for c in range(0, d, chunk):
                    cols = slice(c, c + chunk)
                    h = hrow[s, dst, cols].astype(F32)
                    stage[par, dst, cols] = jnp.where(t < n_seq, h * scale * gains[1:2, cols], h).astype(BF16)
        for kind in (RUN_A, RUN_B):
            gone(kind, t)
        for kind in (RIGHT, LEFT, RIGHT_2, LEFT_2, SIDE):
            go(kind, t)
        mine_copy(t).start()

    def pass_on(t):
        for kind, out in ((RIGHT, FWD_A), (LEFT, FWD_B)):
            arrived(kind, t)
            go(out, t)
        for kind, out in ((RIGHT_2, SIDE_L), (LEFT_2, SIDE_R)):
            arrived(kind, t)
            go(out, t)

    def pass_last(t):
        for kind in (FWD_A, FWD_B):
            arrived(kind, t)
        go(SIDE_2, t)
        mine_copy(t).wait()

    def complete(t):
        for kind in (SIDE_L, SIDE_R, SIDE_2):
            arrived(kind, t)
        for kind in (FWD_A, FWD_B, SIDE_L, SIDE_R, SIDE_2):
            gone(kind, t)

    def back(w, lhs, t, hooks=()):
        @pl.loop(0, n_out)
        def _(n):
            slot = lax.rem(n, 2)
            out_tile(w, n).wait()
            out = _dot(lhs(), dbuf[slot, : w.shape[0], :])
            cols = pl.ds(pl.multiple_of(n * OUT, OUT), OUT)
            own[:, cols] = out[:split]
            oth[:, cols] = out[split:].astype(BF16)
            for piece, _, b in pieces:
                @pl.when(n == b - 1)
                def _():
                    go(piece, t)

            for k, hook in enumerate(hooks):
                @pl.when(n == min(2 * k, n_out - 1))
                def _():
                    hook()

            @pl.when(n + 2 < n_out)
            def _():
                out_tile(w, n + 2).start()

    def norm_rows(first, count):
        narrow = d // 8

        @pl.loop(0, count // 32)
        def _(i):
            here = pl.ds(pl.multiple_of(first + i * 32, 32), 32)
            squares = jnp.zeros((32, narrow), F32)
            for c in range(0, d, narrow):
                v = xb[here, c : c + narrow].astype(F32)
                squares += v * v
            scale = lax.rsqrt(jnp.sum(squares, -1, keepdims=True) / d + EPS)
            for c in range(0, d, narrow):
                cols = slice(c, c + narrow)
                xb[here, cols] = (xb[here, cols].astype(F32) * scale * gains[0:1, cols]).astype(BF16)

    def turned(t):
        return t * cos_ref[...] + pltpu.roll(t, HEAD // 2, 1) * sin_ref[...]

    def project():
        @pl.loop(0, n_wide)
        def _(n):
            on_qkv(n, wait)
            got = _dot(xb[...], wbuf[lax.rem(n, 2)]).astype(BF16).astype(F32)

            @pl.when(n + 2 < n_wide)
            def _():
                on_qkv(n + 2, start)

            for j in range(WIDE // HEAD):
                t = got[:, j * HEAD : (j + 1) * HEAD]
                value = turned(t) if j < WIDE // HEAD - 1 else jnp.where(n < n_wide - 1, turned(t), t)
                hid[:, pl.ds(pl.multiple_of(n * WIDE + j * HEAD, HEAD), HEAD)] = value.astype(BF16)

    def attention():
        block = tokens // 2
        ahead = lax.broadcasted_iota(jnp.int32, (block, block), 1) > lax.broadcasted_iota(jnp.int32, (block, block), 0)

        @pl.loop(0, heads, unroll=2)
        def _(n):
            cols = pl.ds(pl.multiple_of(n * HEAD, HEAD), HEAD)
            for i in range(2):
                q = hid[i * block : (i + 1) * block, cols]
                keys = (i + 1) * block
                scores = lax.dot_general(q, hid[:keys, k_at : k_at + HEAD], (((1,), (1,)), ((), ())), preferred_element_type=F32) * HEAD**-0.5
                last = jnp.where(ahead, -1e30, scores[:, keys - block :])
                scores = last if i == 0 else jnp.concatenate([scores[:, : keys - block], last], 1)
                weights = jnp.exp(scores - jnp.max(scores, -1, keepdims=True))
                total = jnp.sum(weights, -1, keepdims=True)
                seen = (_dot(weights.astype(BF16), hid[:keys, v_at : v_at + HEAD]) / total).astype(BF16)
                for j in range(block // rows):
                    chip, whose = divmod(i * (block // rows) + j, 2)
                    row = pl.multiple_of(lax.rem(whose + core, 2) * split + chip * rows, rows)
                    seen_s[pl.ds(row, rows), cols] = seen[j * rows : (j + 1) * rows]

    first = [pl.ds(k * tokens // 4, tokens // 4) for k in range(4)]
    first = [pltpu.make_async_copy(x_ref.at[0, rows_k], xb.at[rows_k], xsem.at[k]) for k, rows_k in enumerate(first)]
    for copy in first:
        copy.start()
    barrier = pltpu.get_barrier_semaphore()
    for peer in (right, left, other):
        pl.semaphore_signal(barrier, inc=1, device_id=peer, device_id_type=MESH)
    for k, copy in enumerate(first):
        copy.wait()
        if k < min(2, n_wide):
            on_qkv(jnp.int32(k), start)
        norm_rows(k * tokens // 4, tokens // 4)
    for s in range(n_seq):
        row_copy(s).start()
    pl.semaphore_wait(barrier, 3)

    @pl.loop(0, n_seq)
    def _(s):
        t = s - 1
        @pl.when(t >= 0)
        def _():
            spread_far(t)

        @pl.when(t >= 1)
        def _():
            finish(t - 1)

        @pl.when(t >= 0)
        def _():
            spread_near(t)

        @pl.when(s > 0)
        def _():
            x_copy(s).wait()
            norm_rows(0, tokens)

        for n in range(2):
            out_tile(wo, jnp.int32(n)).start()
        project()

        @pl.when(s + 1 < n_seq)
        def _():
            x_copy(s + 1).start()
            for n in range(min(2, n_wide)):
                on_qkv(jnp.int32(n), start)

        @pl.when(s + 1 == n_seq)
        def _():
            for n in range(2):
                on_pair(jnp.int32(n), start)

        @pl.when(t >= 0)
        def _():
            carry_on(t)

        attention()

        @pl.when(t >= 1)
        def _():
            arrived(SIDE, t - 1)

        back(wo, lambda: seen_s[...], s)

        @pl.when(t >= 1)
        def _():
            pass_on(t - 1)

        @pl.when(t >= 2)
        def _():
            pass_last(t - 2)

    def load(m):
        complete(m)
        for copy in b_copies(m):
            copy.start()

    @pl.loop(0, n_seq)
    def _(m):
        t = m + n_seq - 1
        for n in range(2):
            out_tile(w_down, jnp.int32(n)).start()

        @pl.when(m == 0)
        def _():
            load(0)

        spread_far(t)
        finish(t - 1)
        spread_near(t)
        for copy in b_copies(m):
            copy.wait()

        @pl.loop(0, n_ff)
        def _(i):
            on_pair(i, wait)
            both = _dot(xb[...], wbuf[lax.rem(i, 2)])
            hid[:, pl.ds(pl.multiple_of(i * part, part), part)] = (jax.nn.silu(both[:, :part]) * both[:, part:]).astype(BF16)

            @pl.when((i + 2 < n_ff) | (m + 1 < n_seq))
            def _():
                on_pair(lax.rem(i + 2, n_ff), start)

            @pl.when(i == n_ff * 3 // 8)
            def _():
                carry_on(t)

            @pl.when(i == n_ff - 1)
            def _():
                pass_on(t - 1)
                pass_last(t - 2)

        arrived(SIDE, t - 1)

        def ahead(act):
            @pl.when(m + 1 < n_seq)
            def _():
                act()

        back(w_down, lambda: hid[...], t + 1, [lambda: None, lambda: ahead(lambda: load(m + 1))])

    last = jnp.int32(2 * n_seq - 1)
    spread_far(last)
    finish(last - 1)
    spread_near(last)
    carry_on(last)
    arrived(SIDE, last - 1)
    pass_on(last - 1)
    pass_last(last - 2)
    finish(last)
    pass_last(last - 1)
    arrived(SIDE, last)
    pass_on(last)
    pass_last(last)

    @pl.loop(n_seq, 2 * n_seq)
    def _(t):
        complete(t)

    for kind in (FAR_A, NEAR_B, FAR_B, NEAR_A):
        gone(kind, last)
    for t in (last - 1, last):
        for kind in (RIGHT, LEFT, RIGHT_2, LEFT_2, SIDE):
            gone(kind, t)


def _taken(g):
    _, n_seq, tokens, d = g.shape
    cut = 4
    rows = tokens // cut
    places = [(i, pl.ds(j * rows, rows)) for i in range(n_seq) for j in range(cut)]

    def body(src, dst, held, taken, put):
        reads = [pltpu.make_async_copy(src.at[1, i, at], held.at[i, at], taken.at[k]) for k, (i, at) in enumerate(places)]
        writes = [pltpu.make_async_copy(held.at[i, at], dst.at[i, at], put.at[k]) for k, (i, at) in enumerate(places)]
        for read in reads:
            read.start()
        for read, write in zip(reads, writes):
            read.wait()
            write.start()
        for write in writes:
            write.wait()

    hbm = pl.BlockSpec(memory_space=pl.ANY)
    return pl.pallas_call(
        body,
        out_shape=jax.ShapeDtypeStruct((n_seq, tokens, d), g.dtype),
        in_specs=[hbm],
        out_specs=hbm,
        scratch_shapes=[pltpu.VMEM((n_seq, tokens, d), g.dtype), pltpu.SemaphoreType.DMA((len(places),)), pltpu.SemaphoreType.DMA((len(places),))],
        compiler_params=pltpu.CompilerParams(vmem_limit_bytes=60 * 2**20),
    )(g)


def solution(mesh):
    tp = mesh.shape["tp"]
    chips = tp // 2
    assert chips == 4

    def step(x, gain_a, wq, wk, wv, wo, gain_m, w_gate, w_up, w_down):
        n_seq, tokens, d = x.shape
        rows = tokens // tp
        ff = w_down.shape[0]
        angle = np.arange(tokens, dtype=np.float32)[:, None] * np.float32(THETA) ** (-np.arange(HEAD // 2, dtype=np.float32) / (HEAD // 2))
        cos, sin = np.cos(angle), np.sin(angle)
        cos, sin = jnp.asarray(np.concatenate([cos, cos], 1)), jnp.asarray(np.concatenate([-sin, sin], 1))
        gains = jnp.stack([gain_a, gain_m]).astype(F32)
        vmem, hbm = pl.BlockSpec(memory_space=pltpu.VMEM), pl.BlockSpec(memory_space=pl.ANY)
        half = rows // 2
        dma = pltpu.SemaphoreType.DMA
        out = pl.pallas_call(
            _layer,
            out_shape=jax.ShapeDtypeStruct((2 * n_seq, chips, 2, rows, d), BF16),
            in_specs=[hbm, vmem, vmem, vmem] + [hbm] * 7,
            out_specs=hbm,
            scratch_shapes=[
                pltpu.VMEM((tokens, d), BF16),
                pltpu.VMEM((2, d, WIDE), BF16),
                pltpu.VMEM((2, ff, OUT), BF16),
                pltpu.VMEM((tokens // 2, d), F32),
                pltpu.VMEM((tokens // 2, d), BF16),
                pltpu.VMEM((2, tokens // 2, d), BF16),
                pltpu.VMEM((tokens, ff), BF16),
                pltpu.VMEM((tokens, wq.shape[1]), BF16),
                pltpu.VMEM((2, 6, half, d), BF16),
                pltpu.VMEM((4, half, d), BF16),
                pltpu.VMEM((4, half, d), F32),
                pltpu.VMEM((n_seq, rows, d), BF16),
                pltpu.VMEM((2, rows, d), BF16),
                dma((KINDS, 2 * n_seq)), dma((KINDS, 2 * n_seq)),
                dma((2 * chips + 1,)), dma((2, 2)), dma((1,)), dma((2,)), dma((n_seq,)), dma((2 * n_seq,)),
            ],
            compiler_params=pltpu.CompilerParams(collective_id=0, has_side_effects=True, vmem_limit_bytes=62 * 2**20),
        )(x, gains, cos, sin, wq, wk, wv, wo, w_gate, w_up, w_down)
        return _taken(out.reshape(2, n_seq, tokens, d))

    tokens, whole, columns, rows_of = P("dp", None, None), P(None), P(None, "tp"), P("tp", None)
    return jax.shard_map(
        step,
        mesh=mesh,
        in_specs=(tokens, whole, columns, columns, columns, rows_of, whole, columns, columns, rows_of),
        out_specs=tokens,
        check_vma=False,
    )
```

```python
import functools

import jax
import jax.numpy as jnp
import numpy as np
from jax import lax
from jax.experimental import pallas as pl
from jax.experimental.pallas import tpu as pltpu
from jax.sharding import PartitionSpec as P

HEAD = 128
THETA = 10000
EPS = 1e-6
WIDE = 512
OUT = 1024
UNROLL = 3
BF16, F32 = jnp.bfloat16, jnp.float32
MESH = pl.DeviceIdType.MESH
D2D, FAR_A, NEAR_B, FAR_B, NEAR_A, RUN_A, RUN_B, RIGHT, LEFT, SIDE, FWD_A, FWD_B, SIDE_L, SIDE_R, SIDE_2 = range(15)
KINDS = 19
RIGHT_2, LEFT_2 = 17, 18


def _dot(a, b):
    return jnp.dot(a, b, preferred_element_type=F32)


def _layer(x_ref, gain_a, gain_m, cos_ref, sin_ref, wq, wk, wv, wo, w_gate, w_up, w_down, g_ref,
           xb, wbuf, dbuf, own, oth, sib, hid, seen_s, gains, rsr, sbuf, sf, hrow, stage,
           send, recv, xsem, wsem, vsem, dsem, hsem, lsem):
    n_seq, tokens, d = x_ref.shape
    chips, rows = g_ref.shape[1], g_ref.shape[3]
    half = rows // 2
    split = chips * rows
    qw, ff = wq.shape[1], w_down.shape[0]
    heads = qw // HEAD
    k_at, v_at = qw, qw + HEAD
    n_wide, n_out = (qw + 2 * HEAD) // WIDE, d // OUT
    part = WIDE // 2
    n_ff = ff // part
    cuts = sorted({n_out // 2, n_out * 5 // 6, n_out})
    pieces = list(zip((D2D, 15, 16), [0, *cuts], cuts))
    chunk = d // 4

    at = lax.axis_index("tp")
    me, core = at // 2, lax.rem(at, 2)
    rel = lambda k: lax.rem(me + k, chips)
    device = lambda chip: {"tp": chip * 2 + core}
    right, left, other = device(rel(1)), device(rel(chips - 1)), {"tp": me * 2 + 1 - core}

    def x_copy(s):
        return pltpu.make_async_copy(x_ref.at[s], xb, xsem.at[2 * chips])

    def b_copies(m):
        return [pltpu.make_async_copy(g_ref.at[m, k, core if j == 0 else 1 - core], xb.at[pl.ds(j * split + k * rows, rows)],
                                      xsem.at[j * chips + k]) for j in range(2) for k in range(chips)]

    def row_copy(s):
        return pltpu.make_async_copy(x_ref.at[s, pl.ds(pl.multiple_of(at * rows, rows), rows)], hrow.at[s], hsem.at[s])

    def pair(n):
        slot, cols = lax.rem(n, 2), pl.ds(pl.multiple_of(n * part, part), part)
        return [pltpu.make_async_copy(w.at[:, cols], wbuf.at[slot, :, pl.ds(j * part, part)], wsem.at[slot, j])
                for j, w in enumerate((w_gate, w_up))]

    def on_pair(n, act):
        for copy in pair(n):
            act(copy)

    def on_qkv(n, act):
        slot = lax.rem(n, 2)
        rest = WIDE - 2 * HEAD

        @pl.when(n < n_wide - 1)
        def _():
            act(pltpu.make_async_copy(wq.at[:, pl.ds(pl.multiple_of(n * WIDE, WIDE), WIDE)], wbuf.at[slot], wsem.at[slot, 0]))

        @pl.when(n == n_wide - 1)
        def _():
            act(pltpu.make_async_copy(wq.at[:, pl.ds(qw - rest, rest)], wbuf.at[slot, :, pl.ds(0, rest)], wsem.at[slot, 0]))
            act(pltpu.make_async_copy(wk, wbuf.at[slot, :, pl.ds(rest, HEAD)], wsem.at[slot, 1]))
            act(pltpu.make_async_copy(wv, wbuf.at[slot, :, pl.ds(rest + HEAD, HEAD)], vsem.at[0]))

    def out_tile(w, n):
        slot = lax.rem(n, 2)
        return pltpu.make_async_copy(w.at[:, pl.ds(pl.multiple_of(n * OUT, OUT), OUT)], dbuf.at[slot, pl.ds(0, w.shape[0])], dsem.at[slot])

    start, wait = lambda copy: copy.start(), lambda copy: copy.wait()

    def message(kind, t, src, dst, to):
        return pltpu.make_async_remote_copy(src_ref=src, dst_ref=dst, send_sem=send.at[kind, t], recv_sem=recv.at[kind, t],
                                            device_id=to, device_id_type=MESH)

    def sent(kind, t):
        par = lax.rem(t, 2)
        part_a, part_b = pl.ds(0, half), pl.ds(half, half)
        for piece, a, b in pieces:
            if kind == piece:
                cols = pl.ds(a * OUT, (b - a) * OUT)
                return message(kind, t, oth.at[:, cols], sib.at[par, :, cols], other)
        if kind in (FAR_A, NEAR_B, FAR_B, NEAR_A):
            k = kind - FAR_A
            return message(kind, t, sbuf.at[k], rsr.at[par, k], right if k < 2 else left)
        if kind == RUN_A:
            return message(kind, t, rsr.at[par, 0], rsr.at[par, 4], right)
        if kind == RUN_B:
            return message(kind, t, rsr.at[par, 2], rsr.at[par, 5], left)
        mine = g_ref.at[t, me, core]
        if kind == SIDE:
            return message(kind, t, stage.at[par], mine, other)
        if kind in (RIGHT, LEFT_2):
            return message(kind, t, stage.at[par, part_a], g_ref.at[t, me, core, part_a], right if kind == RIGHT else left)
        if kind in (LEFT, RIGHT_2):
            return message(kind, t, stage.at[par, part_b], g_ref.at[t, me, core, part_b], left if kind == LEFT else right)
        if kind == FWD_A:
            ref = g_ref.at[t, rel(chips - 1), core, part_a]
            return message(kind, t, ref, ref, right)
        if kind == FWD_B:
            ref = g_ref.at[t, rel(1), core, part_b]
            return message(kind, t, ref, ref, left)
        ref = g_ref.at[t, rel({SIDE_L: chips - 1, SIDE_R: 1, SIDE_2: 2}[kind]), core]
        return message(kind, t, ref, ref, other)

    def arrived(kind, t):
        par = lax.rem(t, 2)
        part_a, part_b = pl.ds(0, half), pl.ds(half, half)
        cols = [pl.ds(a * OUT, (b - a) * OUT) for piece, a, b in pieces if kind == piece]
        if cols:
            ref, who = sib.at[par, :, cols[0]], other
        elif kind in (FAR_A, NEAR_B, FAR_B, NEAR_A):
            k = kind - FAR_A
            ref, who = rsr.at[par, k], (left if k < 2 else right)
        elif kind == RUN_A:
            ref, who = rsr.at[par, 4], left
        elif kind == RUN_B:
            ref, who = rsr.at[par, 5], right
        elif kind in (RIGHT, RIGHT_2):
            ref, who = g_ref.at[t, rel(chips - 1), core, part_a if kind == RIGHT else part_b], left
        elif kind in (LEFT, LEFT_2):
            ref, who = g_ref.at[t, rel(1), core, part_b if kind == LEFT else part_a], right
        elif kind == FWD_A:
            ref, who = g_ref.at[t, rel(2), core, part_a], left
        elif kind == FWD_B:
            ref, who = g_ref.at[t, rel(2), core, part_b], right
        else:
            ref, who = g_ref.at[t, rel({SIDE: 0, SIDE_L: chips - 1, SIDE_R: 1, SIDE_2: 2}[kind]), 1 - core], other
        message(kind, t, ref, ref, who).wait_recv()

    def go(kind, t):
        sent(kind, t).start()

    def gone(kind, t):
        sent(kind, t).wait_send()

    def mine_copy(t):
        return pltpu.make_async_copy(stage.at[lax.rem(t, 2)], g_ref.at[t, me, core], lsem.at[t])

    def add(t, k, piece, to, slot):
        par, base = lax.rem(t, 2), rel(k) * rows + piece * half

        @pl.loop(0, half // 16)
        def _(i):
            here = pl.ds(pl.multiple_of(base + i * 16, 16), 16)
            for c in range(0, d, chunk):
                total = own[here, c : c + chunk] + sib[par, here, c : c + chunk].astype(F32)
                to[slot, pl.ds(i * 16, 16), c : c + chunk] = total.astype(to.dtype)

    def spread_far(t):
        for piece, _, _ in pieces:
            gone(piece, t)
            arrived(piece, t)

        @pl.when(t >= 1)
        def _():
            for kind in (FAR_A, NEAR_B, FAR_B, NEAR_A):
                gone(kind, t - 1)

        add(t, 2, 0, sbuf, 0)
        go(FAR_A, t)
        add(t, 2, 1, sbuf, 2)
        go(FAR_B, t)

    def spread_near(t):
        add(t, 1, 1, sbuf, 1)
        go(NEAR_B, t)
        add(t, 3, 0, sbuf, 3)
        go(NEAR_A, t)
        add(t, 1, 0, sf, 2)
        add(t, 3, 1, sf, 3)
        add(t, 0, 0, sf, 0)
        add(t, 0, 1, sf, 1)

    def carry_on(t):
        par = lax.rem(t, 2)
        for kind, k, mine, out in ((FAR_A, 0, 2, RUN_A), (FAR_B, 2, 3, RUN_B)):
            arrived(kind, t)

            @pl.loop(0, half // 16)
            def _(i):
                here = pl.ds(i * 16, 16)
                for c in range(0, d, chunk):
                    total = rsr[par, k, here, c : c + chunk].astype(F32) + sf[mine, here, c : c + chunk]
                    rsr[par, k, here, c : c + chunk] = total.astype(BF16)

            go(out, t)

    def finish(t):
        par, s = lax.rem(t, 2), lax.rem(t, n_seq)

        @pl.when(t < n_seq)
        def _():
            row_copy(s).wait()

        @pl.when(t >= 2)
        def _():
            for kind in (RIGHT, LEFT, RIGHT_2, LEFT_2, SIDE):
                gone(kind, t - 2)

        for kind in (NEAR_A, NEAR_B, RUN_A, RUN_B):
            arrived(kind, t)
        for part, (run, near) in enumerate(((4, 3), (5, 1))):
            @pl.loop(0, half // 16)
            def _(i):
                src, dst = pl.ds(i * 16, 16), pl.ds(part * half + i * 16, 16)
                squares = jnp.zeros((16, chunk), F32)
                for c in range(0, d, chunk):
                    cols = slice(c, c + chunk)
                    total = sf[part, src, cols] + rsr[par, run, src, cols].astype(F32) + rsr[par, near, src, cols].astype(F32)
                    h = (hrow[s, dst, cols].astype(F32) + total).astype(BF16)
                    hrow[s, dst, cols] = h
                    squares += h.astype(F32) * h.astype(F32)
                scale = lax.rsqrt(jnp.sum(squares, -1, keepdims=True) / d + EPS)
                for c in range(0, d, chunk):
                    cols = slice(c, c + chunk)
                    h = hrow[s, dst, cols].astype(F32)
                    stage[par, dst, cols] = jnp.where(t < n_seq, h * scale * gains[1:2, cols], h).astype(BF16)
        for kind in (RUN_A, RUN_B):
            gone(kind, t)
        for kind in (RIGHT, LEFT, RIGHT_2, LEFT_2, SIDE):
            go(kind, t)
        mine_copy(t).start()

    def pass_on(t):
        for kind, out in ((RIGHT, FWD_A), (LEFT, FWD_B)):
            arrived(kind, t)
            go(out, t)
        for kind, out in ((RIGHT_2, SIDE_L), (LEFT_2, SIDE_R)):
            arrived(kind, t)
            go(out, t)

    def pass_last(t):
        for kind in (FWD_A, FWD_B):
            arrived(kind, t)
        go(SIDE_2, t)
        mine_copy(t).wait()

    def complete(t):
        for kind in (SIDE_L, SIDE_R, SIDE_2):
            arrived(kind, t)
        for kind in (FWD_A, FWD_B, SIDE_L, SIDE_R, SIDE_2):
            gone(kind, t)

    def back(w, lhs, t, hooks=()):
        @pl.loop(0, n_out)
        def _(n):
            slot = lax.rem(n, 2)
            out_tile(w, n).wait()
            out = _dot(lhs(), dbuf[slot, : w.shape[0], :])
            cols = pl.ds(pl.multiple_of(n * OUT, OUT), OUT)
            own[:, cols] = out[:split]
            oth[:, cols] = out[split:].astype(BF16)
            for piece, _, b in pieces:
                @pl.when(n == b - 1)
                def _():
                    go(piece, t)

            for k, hook in enumerate(hooks):
                @pl.when(n == min(2 * k, n_out - 1))
                def _():
                    hook()

            @pl.when(n + 2 < n_out)
            def _():
                out_tile(w, n + 2).start()

    def norm_rows(first, count):
        narrow = d // 8

        @pl.loop(0, count // 32)
        def _(i):
            here = pl.ds(pl.multiple_of(first + i * 32, 32), 32)
            squares = jnp.zeros((32, narrow), F32)
            for c in range(0, d, narrow):
                v = xb[here, c : c + narrow].astype(F32)
                squares += v * v
            scale = lax.rsqrt(jnp.sum(squares, -1, keepdims=True) / d + EPS)
            for c in range(0, d, narrow):
                cols = slice(c, c + narrow)
                xb[here, cols] = (xb[here, cols].astype(F32) * scale * gains[0:1, cols]).astype(BF16)

    def turned(t):
        return t * cos_ref[...] + pltpu.roll(t, HEAD // 2, 1) * sin_ref[...]

    def project():
        @pl.loop(0, n_wide)
        def _(n):
            on_qkv(n, wait)
            got = _dot(xb[...], wbuf[lax.rem(n, 2)]).astype(BF16).astype(F32)

            @pl.when(n + 2 < n_wide)
            def _():
                on_qkv(n + 2, start)

            for j in range(WIDE // HEAD):
                t = got[:, j * HEAD : (j + 1) * HEAD]
                value = turned(t) if j < WIDE // HEAD - 1 else jnp.where(n < n_wide - 1, turned(t), t)
                hid[:, pl.ds(pl.multiple_of(n * WIDE + j * HEAD, HEAD), HEAD)] = value.astype(BF16)

    def attention():
        block = tokens // 2
        ahead = lax.broadcasted_iota(jnp.int32, (block, block), 1) > lax.broadcasted_iota(jnp.int32, (block, block), 0)

        @pl.loop(0, heads, unroll=UNROLL)
        def _(n):
            cols = pl.ds(pl.multiple_of(n * HEAD, HEAD), HEAD)
            for i in range(2):
                q = hid[i * block : (i + 1) * block, cols]
                keys = (i + 1) * block
                scores = lax.dot_general(q, hid[:keys, k_at : k_at + HEAD], (((1,), (1,)), ((), ())), preferred_element_type=F32) * HEAD**-0.5
                last = jnp.where(ahead, -1e30, scores[:, keys - block :])
                scores = last if i == 0 else jnp.concatenate([scores[:, : keys - block], last], 1)
                weights = jnp.exp(scores - jnp.max(scores, -1, keepdims=True))
                total = jnp.sum(weights, -1, keepdims=True)
                seen = (_dot(weights.astype(BF16), hid[:keys, v_at : v_at + HEAD]) / total).astype(BF16)
                for j in range(block // rows):
                    chip, whose = divmod(i * (block // rows) + j, 2)
                    row = pl.multiple_of(lax.rem(whose + core, 2) * split + chip * rows, rows)
                    seen_s[pl.ds(row, rows), cols] = seen[j * rows : (j + 1) * rows]

    first = [pl.ds(k * tokens // 4, tokens // 4) for k in range(4)]
    first = [pltpu.make_async_copy(x_ref.at[0, rows_k], xb.at[rows_k], xsem.at[k]) for k, rows_k in enumerate(first)]
    for copy in first:
        copy.start()
    for j, gain in enumerate((gain_a, gain_m)):
        wide = gain[...].astype(F32)
        for k in range(d // 128):
            gains[j : j + 1, k * 128 : (k + 1) * 128] = wide[k : k + 1, :]
    barrier = pltpu.get_barrier_semaphore()
    for peer in (right, left, other):
        pl.semaphore_signal(barrier, inc=1, device_id=peer, device_id_type=MESH)
    for k, copy in enumerate(first):
        copy.wait()
        if k < min(2, n_wide):
            on_qkv(jnp.int32(k), start)
        norm_rows(k * tokens // 4, tokens // 4)
    for s in range(n_seq):
        row_copy(s).start()
    pl.semaphore_wait(barrier, 3)

    @pl.loop(0, n_seq)
    def _(s):
        t = s - 1
        @pl.when(t >= 0)
        def _():
            spread_far(t)

        @pl.when(t >= 1)
        def _():
            finish(t - 1)

        @pl.when(t >= 0)
        def _():
            spread_near(t)

        @pl.when(s > 0)
        def _():
            x_copy(s).wait()
            norm_rows(0, tokens)

        for n in range(2):
            out_tile(wo, jnp.int32(n)).start()
        project()

        @pl.when(s + 1 < n_seq)
        def _():
            x_copy(s + 1).start()
            for n in range(min(2, n_wide)):
                on_qkv(jnp.int32(n), start)

        @pl.when(s + 1 == n_seq)
        def _():
            for n in range(2):
                on_pair(jnp.int32(n), start)

        attention()

        @pl.when(t >= 0)
        def _():
            carry_on(t)


        @pl.when(t >= 1)
        def _():
            arrived(SIDE, t - 1)

        back(wo, lambda: seen_s[...], s)

        @pl.when(t >= 1)
        def _():
            pass_on(t - 1)

        @pl.when(t >= 2)
        def _():
            pass_last(t - 2)

    def load(m):
        complete(m)
        for copy in b_copies(m):
            copy.start()

    @pl.loop(0, n_seq)
    def _(m):
        t = m + n_seq - 1
        for n in range(2):
            out_tile(w_down, jnp.int32(n)).start()

        @pl.when(m == 0)
        def _():
            load(0)

        spread_far(t)
        finish(t - 1)
        spread_near(t)
        for copy in b_copies(m):
            copy.wait()

        @pl.loop(0, n_ff)
        def _(i):
            on_pair(i, wait)
            both = _dot(xb[...], wbuf[lax.rem(i, 2)])
            hid[:, pl.ds(pl.multiple_of(i * part, part), part)] = (jax.nn.silu(both[:, :part]) * both[:, part:]).astype(BF16)

            @pl.when((i + 2 < n_ff) | (m + 1 < n_seq))
            def _():
                on_pair(lax.rem(i + 2, n_ff), start)

            @pl.when(i == n_ff * 3 // 8)
            def _():
                carry_on(t)

            @pl.when(i == n_ff - 1)
            def _():
                pass_on(t - 1)
                pass_last(t - 2)

        arrived(SIDE, t - 1)

        def ahead(act):
            @pl.when(m + 1 < n_seq)
            def _():
                act()

        back(w_down, lambda: hid[...], t + 1, [lambda: None, lambda: ahead(lambda: load(m + 1))])

    last = jnp.int32(2 * n_seq - 1)
    spread_far(last)
    finish(last - 1)
    spread_near(last)
    carry_on(last)
    arrived(SIDE, last - 1)
    pass_on(last - 1)
    pass_last(last - 2)
    finish(last)
    pass_last(last - 1)
    arrived(SIDE, last)
    pass_on(last)
    pass_last(last)

    @pl.loop(n_seq, 2 * n_seq)
    def _(t):
        complete(t)

    for kind in (FAR_A, NEAR_B, FAR_B, NEAR_A):
        gone(kind, last)
    for t in (last - 1, last):
        for kind in (RIGHT, LEFT, RIGHT_2, LEFT_2, SIDE):
            gone(kind, t)


def _taken(g):
    _, n_seq, tokens, d = g.shape
    cut = 4
    rows = tokens // cut
    places = [(i, pl.ds(j * rows, rows)) for i in range(n_seq) for j in range(cut)]

    def body(src, dst, held, taken, put):
        reads = [pltpu.make_async_copy(src.at[1, i, at], held.at[i, at], taken.at[k]) for k, (i, at) in enumerate(places)]
        writes = [pltpu.make_async_copy(held.at[i, at], dst.at[i, at], put.at[k]) for k, (i, at) in enumerate(places)]
        for read in reads:
            read.start()
        for read, write in zip(reads, writes):
            read.wait()
            write.start()
        for write in writes:
            write.wait()

    hbm = pl.BlockSpec(memory_space=pl.ANY)
    return pl.pallas_call(
        body,
        out_shape=jax.ShapeDtypeStruct((n_seq, tokens, d), g.dtype),
        in_specs=[hbm],
        out_specs=hbm,
        scratch_shapes=[pltpu.VMEM((n_seq, tokens, d), g.dtype), pltpu.SemaphoreType.DMA((len(places),)), pltpu.SemaphoreType.DMA((len(places),))],
        compiler_params=pltpu.CompilerParams(vmem_limit_bytes=60 * 2**20),
    )(g)


def solution(mesh):
    tp = mesh.shape["tp"]
    chips = tp // 2
    assert chips == 4

    def step(x, gain_a, wq, wk, wv, wo, gain_m, w_gate, w_up, w_down):
        n_seq, tokens, d = x.shape
        rows = tokens // tp
        ff = w_down.shape[0]
        angle = np.arange(tokens, dtype=np.float32)[:, None] * np.float32(THETA) ** (-np.arange(HEAD // 2, dtype=np.float32) / (HEAD // 2))
        cos, sin = np.cos(angle), np.sin(angle)
        cos, sin = jnp.asarray(np.concatenate([cos, cos], 1)), jnp.asarray(np.concatenate([-sin, sin], 1))
        gains = [gain.reshape(d // 128, 128) for gain in (gain_a, gain_m)]
        vmem, hbm = pl.BlockSpec(memory_space=pltpu.VMEM), pl.BlockSpec(memory_space=pl.ANY)
        half = rows // 2
        dma = pltpu.SemaphoreType.DMA
        out = pl.pallas_call(
            _layer,
            out_shape=jax.ShapeDtypeStruct((2 * n_seq, chips, 2, rows, d), BF16),
            in_specs=[hbm, vmem, vmem, vmem, vmem] + [hbm] * 7,
            out_specs=hbm,
            scratch_shapes=[
                pltpu.VMEM((tokens, d), BF16),
                pltpu.VMEM((2, d, WIDE), BF16),
                pltpu.VMEM((2, ff, OUT), BF16),
                pltpu.VMEM((tokens // 2, d), F32),
                pltpu.VMEM((tokens // 2, d), BF16),
                pltpu.VMEM((2, tokens // 2, d), BF16),
                pltpu.VMEM((tokens, ff), BF16),
                pltpu.VMEM((tokens, wq.shape[1]), BF16),
                pltpu.VMEM((2, d), F32),
                pltpu.VMEM((2, 6, half, d), BF16),
                pltpu.VMEM((4, half, d), BF16),
                pltpu.VMEM((4, half, d), F32),
                pltpu.VMEM((n_seq, rows, d), BF16),
                pltpu.VMEM((2, rows, d), BF16),
                dma((KINDS, 2 * n_seq)), dma((KINDS, 2 * n_seq)),
                dma((2 * chips + 1,)), dma((2, 2)), dma((1,)), dma((2,)), dma((n_seq,)), dma((2 * n_seq,)),
            ],
            compiler_params=pltpu.CompilerParams(collective_id=0, has_side_effects=True, vmem_limit_bytes=62 * 2**20),
        )(x, *gains, cos, sin, wq, wk, wv, wo, w_gate, w_up, w_down)
        return _taken(out.reshape(2, n_seq, tokens, d))

    tokens, whole, columns, rows_of = P("dp", None, None), P(None), P(None, "tp"), P("tp", None)
    return jax.shard_map(
        step,
        mesh=mesh,
        in_specs=(tokens, whole, columns, columns, columns, rows_of, whole, columns, columns, rows_of),
        out_specs=tokens,
        check_vma=False,
    )
```
